256 devices in a mesh: section: 8 (over y, z_hi), dp: 32 (over z_lo, x, core).
Axes of the slice: x: 4, y: 4, z: 8 (z_hi: 2, z_lo: 4; z = z_hi * 4 + z_lo), core: 2. Of those that a mesh axis runs over, the one named last changes fastest.
Arguments:
- residuals: float32 [32, 1024, 4096], P('section', 'dp'), may hold values from -100 to 100, as said below
- owners: int32 [256], replicated, may hold values from 0 to 255, each once
Outputs:
- harvest: bfloat16 [1024, 32, 4096], P(('section', 'dp'))
The draws below stay inside these ranges and needn't reach their ends.
Inputs may be any that keep to these rules, and one draw needn't show every extreme that they name: `owners`: a permutation of the block numbers. `residuals`: real-valued activations.
All inputs are finite; a program needn't handle non-finite values.
Results may differ from the reference program's by a relative error of at most 0.0004.
Values may be sent and summed in bfloat16 or wider, within the bound.
A program may use at most 64 MiB of HBM per device.

```python
import math
import jax
import jax.numpy as jnp
from jax import lax

D = 4096
BLOCK = 4
LAYERS = 32
TOK_DEV = 32
TOKENS = 1024
BLOCKS = 256


def draw_residuals(key, part):
    noise_key = jax.random.fold_in(key, 11)
    shard_key = jax.random.fold_in(key, 12)
    token_key = jax.random.fold_in(key, 13)
    offset_key = jax.random.fold_in(key, 14)
    shard_count = TOKENS // TOK_DEV
    base_noise = jax.random.normal(noise_key, (LAYERS, TOKENS, D), jnp.float32)
    log_low = math.log(0.3)
    log_high = math.log(3.0)
    shard_scale = jnp.exp(jax.random.uniform(shard_key, (LAYERS, shard_count, 1, 1), jnp.float32, log_low, log_high))
    token_scale = jax.random.uniform(token_key, (LAYERS, TOKENS, 1), jnp.float32, 0.5, 1.5)
    offset = 2.0 * jax.random.normal(offset_key, (LAYERS, TOKENS, 1), jnp.float32)
    scaled_rows = base_noise.reshape(LAYERS, shard_count, TOK_DEV, D) * shard_scale
    return jnp.clip(scaled_rows.reshape(LAYERS, TOKENS, D) * token_scale + offset, -100.0, 100.0)


def setup_inputs(seed: int = 0) -> dict:
    key_list = jax.random.split(jax.random.key(seed), 3)
    return {
        "residuals": draw_residuals(jax.random.fold_in(key_list[2], 71), 0),
        "owners": jax.random.permutation(key_list[1], BLOCKS).astype(jnp.int32),
    }


def reference(residuals, owners):

    def normalize_layer(layer_rows):
        centered = layer_rows - lax.optimization_barrier(jnp.mean(layer_rows, axis=1, keepdims=True))
        energy = jnp.sum(centered * centered)
        layer_scale = 1.0 / jnp.sqrt(energy / (TOKENS * D) + 1.0)
        return (centered * layer_scale).astype(jnp.bfloat16)
    normed = lax.map(normalize_layer, residuals)
    inverse = jnp.zeros((BLOCKS,), jnp.int32).at[owners.astype(jnp.int32)].set(jnp.arange(BLOCKS, dtype=jnp.int32))
    blocked = normed.reshape(LAYERS, BLOCKS, BLOCK, D)[:, inverse]
    return blocked.transpose(1, 2, 0, 3).reshape(TOKENS, LAYERS, D)
```

```python
import jax
import jax.numpy as jnp
from jax import lax
from jax.experimental import pallas as pl
from jax.experimental.pallas import tpu as pltpu
from jax.sharding import Mesh
from jax.sharding import PartitionSpec as P

AXES = ("y", "zh", "zl", "x", "c")
MESH = pl.DeviceIdType.MESH
F32 = jnp.float32
BF16 = jnp.bfloat16
LANES = 128


def device(y, z, x, c):
    return {"y": y, "zh": lax.div(z, 4), "zl": lax.rem(z, 4), "x": x, "c": c}


def whole(ref, count, sem):
    part = ref.at[pl.ds(0, count)]
    return pltpu.make_async_copy(part, part, sem)


def kernel(
    inverse, x_hbm, out, x_in, rows, energy, plane, plane_sum, line,
    split_a, split_b, mixed_a, mixed_b, sorted_a, sorted_b, got_a, got_b,
    in_sem, y_sem, plane_send, plane_recv, line_send, line_recv,
    one_send, one_recv, two_send, two_recv,
):
    layers, tokens, features = x_in.shape
    y, x, c = lax.axis_index("y"), lax.axis_index("x"), lax.axis_index("c")
    zl = lax.axis_index("zl")
    z = lax.axis_index("zh") * 4 + zl
    column = (zl * 4 + x) * 2 + c
    me = (y * 8 + z) * 8 + x * 2 + c
    split, mixed = (split_a, split_b), (mixed_a, mixed_b)
    ordered, got = (sorted_a, sorted_b), (got_a, got_b)

    loads = [
        pltpu.make_async_copy(x_hbm.at[i], x_in.at[i], in_sem.at[i]) for i in range(layers)
    ]
    for load in loads:
        load.start()

    barrier = pltpu.get_barrier_semaphore()
    for step in (4, 3, 5, 2, 6, 1, 7):
        pl.semaphore_signal(
            barrier, inc=1, device_id=device(y, lax.rem(z + step, 8), x, c), device_id_type=MESH
        )
    for step in (2, 1, 3):
        pl.semaphore_signal(
            barrier, inc=1, device_id=device(lax.rem(y + step, 4), z, x, c), device_id_type=MESH
        )

    def near(i):
        return device(y, z, lax.rem(x + lax.div(i, 2), 4), lax.rem(c + lax.rem(i, 2), 2))

    for step in range(1, 8):
        pl.semaphore_signal(barrier, inc=1, device_id=near(step), device_id_type=MESH)

    energy[...] = jnp.zeros_like(energy)
    for layer in range(layers):
        loads[layer].wait()

        def octet(q, total, layer=layer):
            block = x_in[layer, pl.ds(pl.multiple_of(q * 8, 8), 8), :]
            centered = block - jnp.mean(block, axis=1, keepdims=True)
            for j in range(features // LANES):
                piece = centered[:, j * LANES : (j + 1) * LANES]
                total = total + piece * piece
                rows[j, q, pl.ds(layer, 8, stride=4), :] = piece
            return total

        total = lax.fori_loop(0, tokens // 8, octet, jnp.zeros((8, LANES), F32))
        summed = jnp.sum(total, axis=0, keepdims=True)
        energy[layer : layer + 1, :] = summed
        energy[layer + 4 : layer + 5, :] = summed

    slot = x * 2 + c
    plane[slot] = energy[...]
    pl.semaphore_wait(barrier, 17)

    def send_plane(i, _):
        pltpu.make_async_remote_copy(
            energy, plane.at[slot], plane_send, plane_recv, device_id=near(i), device_id_type=MESH
        ).start()
        return 0

    lax.fori_loop(1, 8, send_plane, 0)
    whole(plane, 7, plane_recv).wait()
    partial = plane[0]
    for i in range(1, 8):
        partial = partial + plane[i]
    plane_sum[...] = partial
    line[zl] = partial
    base = lax.div(z, 4) * 4
    for step in (3, 2, 1):
        pltpu.make_async_remote_copy(
            plane_sum, line.at[zl], line_send, line_recv,
            device_id=device(y, base + lax.rem(zl + step, 4), x, c), device_id_type=MESH,
        ).start()
    for step in (2, 1, 3):
        pl.semaphore_signal(
            y_sem, inc=1, device_id=device(lax.rem(y + step, 4), z, x, c), device_id_type=MESH
        )
    whole(line, 3, line_recv).wait()
    sums = (line[0] + line[1]) + (line[2] + line[3])
    sums = jnp.sum(sums, axis=1, keepdims=True)
    scale = 1.0 / jnp.sqrt(sums / (tokens * 32 * features) + 1.0)
    scale = jnp.broadcast_to(scale, (8, LANES))

    for h in range(2):

        def pack(j, _, h=h):
            for q in range(4):
                for k in range(2):
                    piece = rows[j, q, pl.ds(16 * k + 8 * h, 8), :] * scale
                    split[h][j, 2 * q + k] = piece.astype(BF16)
            return 0

        lax.fori_loop(0, 32, pack, 0)
        mixed[h][pl.ds(pl.multiple_of(column * 8, 8), 8)] = split[h][column]
        for near_by in (2, 1, 3, 0):

            def send_one(i, _, h=h, near_by=near_by):
                dx = lax.div(i, 2)
                tx, tc = lax.rem(x + dx, 4), lax.rem(c + lax.rem(i, 2), 2)
                if near_by == 2:
                    tz = lax.rem(z + 2 + 4 * lax.rem(dx + h, 2), 8)
                else:
                    tz = lax.rem(z + (0, 1, 2, 7)[near_by], 8)
                target = (lax.rem(zl + near_by, 4) * 4 + tx) * 2 + tc
                pltpu.make_async_remote_copy(
                    split[h].at[target],
                    mixed[h].at[pl.ds(pl.multiple_of(column * 8, 8), 8)],
                    one_send.at[h], one_recv.at[h],
                    device_id=device(y, tz, tx, tc), device_id_type=MESH,
                ).start()
                return 0

            lax.fori_loop(1 if near_by == 0 else 0, 8, send_one, 0)

    pl.semaphore_wait(y_sem, 3)
    for h in range(2):
        whole(mixed[h], 248, one_recv.at[h]).wait()

        def order(o, _, h=h):
            ordered[h][o] = mixed[h][inverse[o]]
            return 0

        lax.fori_loop(0, 256, order, 0, unroll=8)
        got[h][me] = ordered[h][me]

        def send_two(i, _, h=h):
            ty = lax.rem(y + lax.rem(lax.div(i, 8), 4), 4)
            tz = lax.rem(z + lax.rem(i, 8), 8)
            tx = lax.rem(x + lax.rem(lax.div(i, 32), 4), 4)
            tc = lax.rem(c + lax.div(i, 128), 2)
            target = (ty * 8 + tz) * 8 + tx * 2 + tc
            pltpu.make_async_remote_copy(
                ordered[h].at[target], got[h].at[me], two_send.at[h], two_recv.at[h],
                device_id=device(ty, tz, tx, tc), device_id_type=MESH,
            ).start()
            return 0

        lax.fori_loop(1, 256, send_two, 0)

    block = inverse[me]
    from_z, from_x = lax.div(block, 64), lax.rem(lax.div(block, 16), 4)
    low = lax.broadcasted_iota(jnp.int32, (8, LANES), 0) < 4
    for h in range(2):
        whole(got[h], 255, two_recv.at[h]).wait()

        def place(j, _, h=h):
            away = lax.rem(lax.div(j, 8) - from_z + 4, 4)
            odd = lax.rem(lax.rem(lax.div(j, 2), 4) - from_x + 4 + h, 2)
            move = jnp.where(
                away == 0, 0, jnp.where(away == 1, 1, jnp.where(away == 3, 7, 2 + 4 * odd))
            )
            half = lax.div(lax.rem(from_z + move, 8), 4)
            at = pl.ds(pl.multiple_of(j * LANES, LANES), LANES)
            for k in range(4):
                first = got[h][k * 64 + half * 32 + j].astype(F32)
                second = got[h][k * 64 + (1 - half) * 32 + j].astype(F32)
                upper = jnp.where(low, first, pltpu.roll(second, 4, 0))
                lower = jnp.where(low, pltpu.roll(first, 4, 0), second)
                out[2 * h, pl.ds(8 * k, 8), at] = upper.astype(BF16)
                out[2 * h + 1, pl.ds(8 * k, 8), at] = lower.astype(BF16)
            return 0

        lax.fori_loop(0, 32, place, 0)

    whole(plane, 7, plane_send).wait()
    whole(line, 3, line_send).wait()
    for h in range(2):
        whole(mixed[h], 248, one_send.at[h]).wait()
        whole(got[h], 255, two_send.at[h]).wait()


def on_device(residuals, owners):
    layers, tokens, features = residuals.shape
    blocks = owners.shape[0]
    numbers = jnp.arange(blocks, dtype=jnp.int32)
    inverse = jnp.sum(
        jnp.where(owners[None, :] == numbers[:, None], numbers[None, :], 0), axis=1
    )
    dma = pltpu.SemaphoreType.DMA
    vmem = pltpu.VMEM
    return pl.pallas_call(
        kernel,
        out_shape=jax.ShapeDtypeStruct((4, 8 * layers, features), BF16),
        in_specs=[
            pl.BlockSpec(memory_space=pltpu.SMEM),
            pl.BlockSpec(memory_space=pl.ANY),
        ],
        out_specs=pl.BlockSpec(memory_space=pltpu.VMEM),
        scratch_shapes=[
            vmem((layers, tokens, features), F32),
            vmem((32, 4, 32, LANES), F32),
            vmem((8, LANES), F32),
            vmem((8, 8, LANES), F32),
            vmem((8, LANES), F32),
            vmem((4, 8, LANES), F32),
            vmem((32, 8, 8, LANES), BF16),
            vmem((32, 8, 8, LANES), BF16),
            vmem((blocks, 8, LANES), BF16),
            vmem((blocks, 8, LANES), BF16),
            vmem((blocks, 8, LANES), BF16),
            vmem((blocks, 8, LANES), BF16),
            vmem((blocks, 8, LANES), BF16),
            vmem((blocks, 8, LANES), BF16),
            dma((layers,)),
            pltpu.SemaphoreType.REGULAR,
            dma, dma, dma, dma,
            dma((2,)), dma((2,)), dma((2,)), dma((2,)),
        ],
        compiler_params=pltpu.CompilerParams(collective_id=0, has_side_effects=True),
    )(inverse, residuals)


def solution(mesh):
    split = Mesh(mesh.devices.reshape(4, 2, 4, 4, 2), AXES)
    return jax.shard_map(
        on_device,
        mesh=split,
        in_specs=(P(("y", "zh"), ("zl", "x", "c"), None), P()),
        out_specs=P(AXES, None, None),
        check_vma=False,
    )
```

```python
import jax
import jax.numpy as jnp
from jax import lax
from jax.experimental import pallas as pl
from jax.experimental.pallas import tpu as pltpu
from jax.sharding import PartitionSpec as P

MESH = pl.DeviceIdType.MESH
F32 = jnp.float32
BF16 = jnp.bfloat16
LANES = 128


def device(number):
    return {"section": lax.div(number, 32), "dp": lax.rem(number, 32)}


def whole(ref, count, sem):
    part = ref.at[pl.ds(0, count)]
    return pltpu.make_async_copy(part, part, sem)


def kernel(
    owners_hbm, x_hbm, out, owners, inverse, found, x_in, sums, means, rows, energy, plane,
    plane_sum, line, split_a, split_b, mixed_a, mixed_b, sorted_a, sorted_b, got_a, got_b,
    in_sem, own_sem, y_sem, plane_send, plane_recv, line_send, line_recv,
    one_send, one_recv, two_send, two_recv,
):
    layers, tokens, features = x_in.shape
    octets, slices = tokens // 8, features // LANES
    section, column = lax.axis_index("section"), lax.axis_index("dp")
    y, zh = lax.div(section, 2), lax.rem(section, 2)
    zl, slot = lax.div(column, 8), lax.rem(column, 8)
    z = zh * 4 + zl
    x = lax.div(slot, 2)
    me = section * 32 + column
    split, mixed = (split_a, split_b), (mixed_a, mixed_b)
    ordered, got = (sorted_a, sorted_b), (got_a, got_b)

    loads = [
        pltpu.make_async_copy(x_hbm.at[i], x_in.at[i], in_sem.at[i]) for i in range(layers)
    ]
    for load in loads:
        load.start()
    fetch = pltpu.make_async_copy(owners_hbm, owners, own_sem.at[0])
    fetch.start()

    def signal(sem, target):
        pl.semaphore_signal(sem, inc=1, device_id=device(target), device_id_type=MESH)

    barrier = pltpu.get_barrier_semaphore()
    for step in (3, 5, 2, 6, 1, 7):
        signal(barrier, y * 64 + lax.rem(z + step, 8) * 8 + slot)
    for step in (2, 1, 3):
        signal(barrier, lax.rem(y + step, 4) * 64 + z * 8 + slot)
    for step in range(1, 8):
        signal(barrier, y * 64 + z * 8 + lax.rem(slot + step, 8))

    for layer in range(layers):
        loads[layer].wait()

        def add_up(q, _, layer=layer):
            at = pl.ds(pl.multiple_of(q * 8, 8), 8)
            parts = [x_in[layer, at, j * LANES : (j + 1) * LANES] for j in range(slices)]
            while len(parts) > 1:
                parts = [a + b for a, b in zip(parts[::2], parts[1::2])]
            sums[layer * octets + q] = parts[0]
            return 0

        lax.fori_loop(0, octets, add_up, 0)
    mean = jnp.sum(sums[...], axis=2, keepdims=True) / features
    means[...] = jnp.broadcast_to(mean, means.shape)

    for layer in range(layers):

        def squares(q, totals, layer=layer):
            at = pl.ds(pl.multiple_of(q * 8, 8), 8)
            mean = means[layer * octets + q]
            totals = list(totals)
            for j in range(slices):
                piece = x_in[layer, at, j * LANES : (j + 1) * LANES] - mean
                totals[j % 4] = totals[j % 4] + piece * piece
            return tuple(totals)

        zero = jnp.zeros((8, LANES), F32)
        totals = lax.fori_loop(0, octets, squares, (zero,) * 4)
        total = (totals[0] + totals[1]) + (totals[2] + totals[3])
        summed = jnp.sum(total, axis=0, keepdims=True)
        energy[layer : layer + 1, :] = summed
        energy[layer + 4 : layer + 5, :] = summed

    plane[slot] = energy[...]
    pl.semaphore_wait(barrier, 16)
    for step in range(1, 8):
        pltpu.make_async_remote_copy(
            energy, plane.at[slot], plane_send, plane_recv,
            device_id=device(y * 64 + z * 8 + lax.rem(slot + step, 8)), device_id_type=MESH,
        ).start()

    for layer in range(layers):

        def arrange(q, _, layer=layer):
            at = pl.ds(pl.multiple_of(q * 8, 8), 8)
            mean = means[layer * octets + q]
            for j in range(slices):
                piece = x_in[layer, at, j * LANES : (j + 1) * LANES] - mean
                rows[j, q, pl.ds(layer, 8, stride=4), :] = piece
            return 0

        lax.fori_loop(0, octets, arrange, 0)

    whole(plane, 7, plane_recv).wait()
    partial = plane[0]
    for i in range(1, 8):
        partial = partial + plane[i]
    plane_sum[...] = partial
    line[zl] = partial
    for step in (3, 2, 1):
        pltpu.make_async_remote_copy(
            plane_sum, line.at[zl], line_send, line_recv,
            device_id=device(y * 64 + zh * 32 + lax.rem(zl + step, 4) * 8 + slot), device_id_type=MESH,
        ).start()
    for step in (2, 1, 3):
        signal(y_sem, lax.rem(y + step, 4) * 64 + z * 8 + slot)
    whole(line, 3, line_recv).wait()
    total = (line[0] + line[1]) + (line[2] + line[3])
    total = jnp.sum(total, axis=1, keepdims=True)
    scale = 1.0 / jnp.sqrt(total / (tokens * 32 * features) + 1.0)
    scale = jnp.broadcast_to(scale, (8, LANES))

    my_blocks = pl.ds(pl.multiple_of(column * 8, 8), 8)
    for h in range(2):
        for away in (2, 1, 3, 0):
            first = lax.rem(zl + away, 4) * 8

            def pack(i, _, h=h, first=first):
                for q in range(octets):
                    for k in range(2):
                        piece = rows[first + i, q, pl.ds(16 * k + 8 * h, 8), :] * scale
                        split[h][first + i, 2 * q + k] = piece.astype(BF16)
                return 0

            lax.fori_loop(0, 8, pack, 0)
            for i in range(1 if away == 0 else 0, 8):
                there = lax.rem(slot + i, 8)
                if away == 2:
                    odd = lax.rem(lax.div(there, 2) + x + h, 2)
                    tz = lax.rem(z + 2 + 4 * odd, 8)
                else:
                    tz = lax.rem(z + (0, 1, 2, 7)[away], 8)
                pltpu.make_async_remote_copy(
                    split[h].at[first + there], mixed[h].at[my_blocks],
                    one_send.at[h], one_recv.at[h],
                    device_id=device(y * 64 + tz * 8 + there), device_id_type=MESH,
                ).start()
        mixed[h][my_blocks] = split[h][column]

    fetch.wait()
    numbers = (
        lax.broadcasted_iota(jnp.int32, (8, LANES), 0) * LANES
        + lax.broadcasted_iota(jnp.int32, (8, LANES), 1)
    )

    def invert(b, known):
        return jnp.where(numbers == owners[b], b, known)

    found[...] = lax.fori_loop(0, 256, invert, jnp.zeros((8, LANES), jnp.int32), unroll=8)
    pl.semaphore_wait(y_sem, 3)
    table = pltpu.make_async_copy(found, inverse, own_sem.at[1])
    table.start()
    table.wait()

    for h in range(2):
        whole(mixed[h], 248, one_recv.at[h]).wait()
        for top in range(2):

            def order(o, _, h=h, top=top):
                ordered[h][top * LANES + o] = mixed[h][inverse[top, o]]
                return 0

            lax.fori_loop(0, LANES, order, 0, unroll=8)

        def send_two(i, _, h=h):
            target = lax.rem(me + i, 256)
            pltpu.make_async_remote_copy(
                ordered[h].at[target], got[h].at[me], two_send.at[h], two_recv.at[h],
                device_id=device(target), device_id_type=MESH,
            ).start()
            return 0

        lax.fori_loop(1, 256, send_two, 0)
        got[h][me] = ordered[h][me]

    block = inverse[lax.div(me, LANES), lax.rem(me, LANES)]
    from_z, from_x = lax.div(block, 64), lax.rem(lax.div(block, 2 * 8), 4)
    low = lax.broadcasted_iota(jnp.int32, (8, LANES), 0) < 4
    for h in range(2):
        whole(got[h], 255, two_recv.at[h]).wait()

        def place(j, _, h=h):
            away = lax.rem(lax.div(j, 8) - from_z + 4, 4)
            odd = lax.rem(lax.rem(lax.div(j, 2), 4) - from_x + 4 + h, 2)
            move = jnp.where(
                away == 0, 0, jnp.where(away == 1, 1, jnp.where(away == 3, 7, 2 + 4 * odd))
            )
            half = lax.div(lax.rem(from_z + move, 8), 4)
            at = pl.ds(pl.multiple_of(j * LANES, LANES), LANES)
            for k in range(4):
                first = got[h][k * 64 + half * 32 + j].astype(F32)
                second = got[h][k * 64 + (1 - half) * 32 + j].astype(F32)
                upper = jnp.where(low, first, pltpu.roll(second, 4, 0))
                lower = jnp.where(low, pltpu.roll(first, 4, 0), second)
                out[2 * h, pl.ds(8 * k, 8), at] = upper.astype(BF16)
                out[2 * h + 1, pl.ds(8 * k, 8), at] = lower.astype(BF16)
            return 0

        lax.fori_loop(0, slices, place, 0)

    whole(plane, 7, plane_send).wait()
    whole(line, 3, line_send).wait()
    for h in range(2):
        whole(mixed[h], 248, one_send.at[h]).wait()
        whole(got[h], 255, two_send.at[h]).wait()


def on_device(residuals, owners):
    layers, tokens, features = residuals.shape
    blocks = owners.shape[0]
    dma, vmem = pltpu.SemaphoreType.DMA, pltpu.VMEM
    tile = vmem((8, LANES), F32)
    pieces = vmem((blocks, 8, LANES), BF16)
    octets = layers * tokens // 8
    return pl.pallas_call(
        kernel,
        out_shape=jax.ShapeDtypeStruct((4, 8 * layers, features), BF16),
        in_specs=[pl.BlockSpec(memory_space=pltpu.HBM)] * 2,
        out_specs=pl.BlockSpec(memory_space=pltpu.VMEM),
        scratch_shapes=[
            pltpu.SMEM((blocks,), jnp.int32),
            pltpu.SMEM((8, LANES), jnp.int32),
            vmem((8, LANES), jnp.int32),
            vmem((layers, tokens, features), F32),
            vmem((octets, 8, LANES), F32),
            vmem((octets, 8, LANES), F32),
            vmem((features // LANES, tokens // 8, 32, LANES), F32),
            tile,
            vmem((8, 8, LANES), F32),
            tile,
            vmem((4, 8, LANES), F32),
            vmem((32, 8, 8, LANES), BF16),
            vmem((32, 8, 8, LANES), BF16),
            pieces, pieces, pieces, pieces, pieces, pieces,
            dma((layers,)),
            dma((2,)),
            pltpu.SemaphoreType.REGULAR,
            dma, dma, dma, dma,
            dma((2,)), dma((2,)), dma((2,)), dma((2,)),
        ],
        compiler_params=pltpu.CompilerParams(
            collective_id=0, has_side_effects=True, vmem_limit_bytes=16 * 2**20
        ),
    )(*(pltpu.with_memory_space_constraint(a, pltpu.HBM) for a in (owners, residuals)))


def solution(mesh):
    return jax.shard_map(
        on_device,
        mesh=mesh,
        in_specs=(P("section", "dp", None), P()),
        out_specs=P(("section", "dp"), None, None),
        check_vma=False,
    )
```

```python
import jax
import jax.numpy as jnp
from jax import lax
from jax.experimental import pallas as pl
from jax.experimental.pallas import tpu as pltpu
from jax.sharding import PartitionSpec as P

MESH = pl.DeviceIdType.MESH
F32 = jnp.float32
BF16 = jnp.bfloat16
LANES = 128
EARLY = ((0, 0), (0, 1), (1, 0), (3, 0))
FIRST = 2
LATE = 248 - 16 * len(EARLY)


def device(number):
    return {"section": lax.div(number, 32), "dp": lax.rem(number, 32)}


def whole(ref, count, sem):
    part = ref.at[pl.ds(0, count)]
    return pltpu.make_async_copy(part, part, sem)


def kernel(
    owners_hbm, x_hbm, out, owners, inverse, found, x_in, sums, means, rows, energy, plane,
    plane_sum, line, scales, ahead, early, split_a, split_b, mixed_a, mixed_b, sorted_a, sorted_b, got_a, got_b,
    in_sem, own_sem, y_sem, plane_send, plane_recv, line_send, line_recv,
    scale_send, scale_recv, early_send, early_recv,
    one_send, one_recv, two_send, two_recv,
):
    layers, tokens, features = x_in.shape
    octets, slices = tokens // 8, features // LANES
    section, column = lax.axis_index("section"), lax.axis_index("dp")
    y, zh = lax.div(section, 2), lax.rem(section, 2)
    zl, slot = lax.div(column, 8), lax.rem(column, 8)
    z = zh * 4 + zl
    x, c = lax.div(slot, 2), lax.rem(slot, 2)
    me = section * 32 + column
    split, mixed = (split_a, split_b), (mixed_a, mixed_b)
    ordered, got = (sorted_a, sorted_b), (got_a, got_b)

    loads = [
        pltpu.make_async_copy(x_hbm.at[i], x_in.at[i], in_sem.at[i]) for i in range(layers)
    ]
    for load in loads:
        load.start()
    fetch = pltpu.make_async_copy(owners_hbm, owners, own_sem.at[0])
    fetch.start()

    def signal(sem, target):
        pl.semaphore_signal(sem, inc=1, device_id=device(target), device_id_type=MESH)

    barrier = pltpu.get_barrier_semaphore()
    for step in (3, 5, 2, 6, 1, 7):
        signal(barrier, y * 64 + lax.rem(z + step, 8) * 8 + slot)
    for step in (2, 1, 3):
        signal(barrier, lax.rem(y + step, 4) * 64 + z * 8 + slot)
    for step in (1, 7):
        signal(barrier, y * 64 + lax.rem(z + step, 8) * 8 + x * 2 + 1 - c)
    for step in range(1, 8):
        signal(barrier, y * 64 + z * 8 + lax.rem(slot + step, 8))

    for layer in range(layers):
        loads[layer].wait()

        def add_up(q, _, layer=layer):
            at = pl.ds(pl.multiple_of(q * 8, 8), 8)
            parts = [x_in[layer, at, j * LANES : (j + 1) * LANES] for j in range(slices)]
            while len(parts) > 1:
                parts = [a + b for a, b in zip(parts[::2], parts[1::2])]
            sums[layer * octets + q] = parts[0]
            return 0

        lax.fori_loop(0, octets, add_up, 0)
    mean = jnp.sum(sums[...], axis=2, keepdims=True) / features
    means[...] = jnp.broadcast_to(mean, means.shape)

    for layer in range(layers):

        def squares(q, totals, layer=layer):
            at = pl.ds(pl.multiple_of(q * 8, 8), 8)
            mean = means[layer * octets + q]
            totals = list(totals)
            for j in range(slices):
                piece = x_in[layer, at, j * LANES : (j + 1) * LANES] - mean
                totals[j % 4] = totals[j % 4] + piece * piece
            return tuple(totals)

        zero = jnp.zeros((8, LANES), F32)
        totals = lax.fori_loop(0, octets, squares, (zero,) * 4)
        total = (totals[0] + totals[1]) + (totals[2] + totals[3])
        summed = jnp.sum(total, axis=0, keepdims=True)
        energy[layer : layer + 1, :] = summed
        energy[layer + 4 : layer + 5, :] = summed

    plane[slot] = energy[...]
    pl.semaphore_wait(barrier, 18)
    for step in range(1, 8):
        pltpu.make_async_remote_copy(
            energy, plane.at[slot], plane_send, plane_recv,
            device_id=device(y * 64 + z * 8 + lax.rem(slot + step, 8)), device_id_type=MESH,
        ).start()

    def arrange(j, into):
        lanes = pl.ds(pl.multiple_of(j * LANES, LANES), LANES)
        for layer in range(layers):
            for q in range(octets):
                piece = x_in[layer, q * 8 : q * 8 + 8, lanes] - means[layer * octets + q]
                into[q, pl.ds(layer, 8, stride=4), :] = piece

    def slot_at(dx, dc):
        return lax.rem(x + dx, 4) * 2 + lax.rem(c + dc, 2)

    def send_early(steps):
        for k in steps:
            there = slot_at(*EARLY[k])
            for i, (away, move) in enumerate(((1, 1), (3, 7))):
                source = rows.at[lax.rem(zl + away, 4) * 8 + there]
                pltpu.make_async_remote_copy(
                    ahead.at[2 * k + i] if k < FIRST else source, early.at[2 * k + i],
                    early_send, early_recv,
                    device_id=device(y * 64 + lax.rem(z + move, 8) * 8 + there),
                    device_id_type=MESH,
                ).start()

    for k in range(FIRST):
        for i, away in enumerate((1, 3)):
            arrange(lax.rem(zl + away, 4) * 8 + slot_at(*EARLY[k]), ahead.at[2 * k + i])
    send_early(range(FIRST))

    def arrange_all(j, _):
        arrange(j, rows.at[j])
        return 0

    lax.fori_loop(0, slices, arrange_all, 0)

    whole(plane, 7, plane_recv).wait()
    partial = plane[0]
    for i in range(1, 8):
        partial = partial + plane[i]
    plane_sum[...] = partial
    line[zl] = partial
    for step in (3, 2, 1):
        pltpu.make_async_remote_copy(
            plane_sum, line.at[zl], line_send, line_recv,
            device_id=device(y * 64 + zh * 32 + lax.rem(zl + step, 4) * 8 + slot), device_id_type=MESH,
        ).start()
    send_early(range(FIRST, len(EARLY)))
    for step in (2, 1, 3):
        signal(y_sem, lax.rem(y + step, 4) * 64 + z * 8 + slot)
    fetch.wait()
    numbers = (
        lax.broadcasted_iota(jnp.int32, (8, LANES), 0) * LANES
        + lax.broadcasted_iota(jnp.int32, (8, LANES), 1)
    )

    def invert(b, known):
        return jnp.where(numbers == owners[b], b, known)

    found[...] = lax.fori_loop(0, 256, invert, jnp.zeros((8, LANES), jnp.int32), unroll=8)
    table = pltpu.make_async_copy(found, inverse, own_sem.at[1])
    table.start()
    whole(line, 3, line_recv).wait()
    total = (line[0] + line[1]) + (line[2] + line[3])
    total = jnp.sum(total, axis=1, keepdims=True)
    scale = 1.0 / jnp.sqrt(total / (tokens * 32 * features) + 1.0)
    scale = jnp.broadcast_to(scale, (8, LANES))
    scales[2] = scale

    my_blocks = pl.ds(pl.multiple_of(column * 8, 8), 8)
    for h in range(2):
        if h == 1: whole(mixed[0], LATE, one_send.at[0]).wait()
        for away in (2, 1, 3, 0):
            first = lax.rem(zl + away, 4) * 8

            def pack(i, _, h=h, first=first):
                for q in range(octets):
                    for k in range(2):
                        piece = rows[first + i, q, pl.ds(16 * k + 8 * h, 8), :] * scale
                        split[h][first + i, 2 * q + k] = piece.astype(BF16)
                return 0

            lax.fori_loop(0, 8, pack, 0)
            if h == 0 and away == 2:
                for i, move in enumerate((1, 7)):
                    pltpu.make_async_remote_copy(
                        scales.at[2], scales.at[i], scale_send, scale_recv,
                        device_id=device(y * 64 + lax.rem(z + move, 8) * 8 + slot),
                        device_id_type=MESH,
                    ).start()
            for dx, dc in ((2, 0), (2, 1), (1, 0), (3, 0), (1, 1), (3, 1), (0, 1), (0, 0)):
                if (away == 0 and dx + dc == 0) or (away in (1, 3) and (dx, dc) in EARLY):
                    continue
                there = slot_at(dx, dc)
                if away == 2:
                    tz = lax.rem(z + 2 + 4 * ((dx + h) % 2), 8)
                else:
                    tz = lax.rem(z + (0, 1, 2, 7)[away], 8)
                pltpu.make_async_remote_copy(
                    split[h].at[first + there], mixed[h].at[my_blocks],
                    one_send.at[h], one_recv.at[h],
                    device_id=device(y * 64 + tz * 8 + there), device_id_type=MESH,
                ).start()
        mixed[h][my_blocks] = split[h][column]

    table.wait()
    pl.semaphore_wait(y_sem, 3)
    whole(scales, 2, scale_recv).wait()
    whole(early, 2 * len(EARLY), early_recv).wait()
    for h in range(2):
        for k, (dx, dc) in enumerate(EARLY):
            for i, away in enumerate((3, 1)):
                source = lax.rem(zl + away, 4) * 8 + slot_at((4 - dx) % 4, dc)
                for q in range(octets):
                    for part in range(2):
                        low = 16 * part + 8 * h
                        piece = early[2 * k + i, q, low : low + 8, :] * scales[i]
                        mixed[h][source * 8 + 2 * q + part] = piece.astype(BF16)
        whole(mixed[h], LATE, one_recv.at[h]).wait()
        for top in range(2):

            def order(o, _, h=h, top=top):
                ordered[h][top * LANES + o] = mixed[h][inverse[top, o]]
                return 0

            lax.fori_loop(0, LANES, order, 0, unroll=8)

        def send_two(i, _, h=h):
            target = lax.rem(me + i, 256)
            pltpu.make_async_remote_copy(
                ordered[h].at[target], got[h].at[me], two_send.at[h], two_recv.at[h],
                device_id=device(target), device_id_type=MESH,
            ).start()
            return 0

        lax.fori_loop(1, 256, send_two, 0)
        got[h][me] = ordered[h][me]

    block = inverse[lax.div(me, LANES), lax.rem(me, LANES)]
    from_z, from_x = lax.div(block, 64), lax.rem(lax.div(block, 2 * 8), 4)
    low = lax.broadcasted_iota(jnp.int32, (8, LANES), 0) < 4
    for h in range(2):
        whole(got[h], 255, two_recv.at[h]).wait()

        def place(there, _, h=h):
            away = lax.rem(there - from_z + 4, 4)
            for odd in range(2):
                far = lax.rem(odd + from_x + h, 2)
                move = jnp.where(away == 3, 7, jnp.where(away == 2, 2 + 4 * far, away))
                half = lax.div(lax.rem(from_z + move, 8), 4)
                for k in range(4):
                    near_at = k * 64 + half * 32 + there * 8
                    far_at = k * 64 + (1 - half) * 32 + there * 8
                    for i in (2 * odd, 2 * odd + 1, 2 * odd + 4, 2 * odd + 5):
                        at = pl.ds(pl.multiple_of((there * 8 + i) * LANES, LANES), LANES)
                        first = got[h][near_at + i].astype(F32)
                        second = got[h][far_at + i].astype(F32)
                        upper = jnp.where(low, first, pltpu.roll(second, 4, 0))
                        lower = jnp.where(low, pltpu.roll(first, 4, 0), second)
                        out[2 * h, pl.ds(8 * k, 8), at] = upper.astype(BF16)
                        out[2 * h + 1, pl.ds(8 * k, 8), at] = lower.astype(BF16)
            return 0

        lax.fori_loop(0, 4, place, 0)

    whole(plane, 7, plane_send).wait()
    whole(line, 3, line_send).wait()
    whole(scales, 2, scale_send).wait()
    whole(early, 2 * len(EARLY), early_send).wait()
    for h in range(2):
        if h == 1: whole(mixed[h], LATE, one_send.at[h]).wait()
        whole(got[h], 255, two_send.at[h]).wait()


def on_device(residuals, owners):
    layers, tokens, features = residuals.shape
    blocks = owners.shape[0]
    dma, vmem = pltpu.SemaphoreType.DMA, pltpu.VMEM
    tile = vmem((8, LANES), F32)
    pieces = vmem((blocks, 8, LANES), BF16)
    octets = layers * tokens // 8
    return pl.pallas_call(
        kernel,
        out_shape=jax.ShapeDtypeStruct((4, 8 * layers, features), BF16),
        in_specs=[pl.BlockSpec(memory_space=pltpu.HBM)] * 2,
        out_specs=pl.BlockSpec(memory_space=pltpu.VMEM),
        scratch_shapes=[
            pltpu.SMEM((blocks,), jnp.int32),
            pltpu.SMEM((8, LANES), jnp.int32),
            vmem((8, LANES), jnp.int32),
            vmem((layers, tokens, features), F32),
            vmem((octets, 8, LANES), F32),
            vmem((octets, 8, LANES), F32),
            vmem((features // LANES, tokens // 8, 32, LANES), F32),
            tile,
            vmem((8, 8, LANES), F32),
            tile,
            vmem((4, 8, LANES), F32),
            vmem((3, 8, LANES), F32),
            vmem((2 * FIRST, tokens // 8, 32, LANES), F32),
            vmem((2 * len(EARLY), tokens // 8, 32, LANES), F32),
            vmem((32, 8, 8, LANES), BF16),
            vmem((32, 8, 8, LANES), BF16),
            pieces, pieces, pieces, pieces, pieces, pieces,
            dma((layers,)),
            dma((2,)),
            pltpu.SemaphoreType.REGULAR,
            dma, dma, dma, dma, dma, dma, dma, dma,
            dma((2,)), dma((2,)), dma((2,)), dma((2,)),
        ],
        compiler_params=pltpu.CompilerParams(
            collective_id=0, has_side_effects=True, vmem_limit_bytes=16 * 2**20
        ),
    )(*(pltpu.with_memory_space_constraint(a, pltpu.HBM) for a in (owners, residuals)))


def solution(mesh):
    return jax.shard_map(
        on_device,
        mesh=mesh,
        in_specs=(P("section", "dp", None), P()),
        out_specs=P(("section", "dp"), None, None),
        check_vma=False,
    )
```

```python
import jax
import jax.numpy as jnp
from jax import lax
from jax.experimental import pallas as pl
from jax.experimental.pallas import tpu as pltpu
from jax.sharding import PartitionSpec as P

MESH = pl.DeviceIdType.MESH
F32 = jnp.float32
BF16 = jnp.bfloat16
LANES = 128
EARLY = ((0, 0), (0, 1), (1, 0), (3, 1))
FIRST = 2
FRONT = 1
RATE = 2
LATE = 248 - 16 * len(EARLY)


def device(number):
    return {"section": lax.div(number, 32), "dp": lax.rem(number, 32)}


def whole(ref, count, sem):
    part = ref.at[pl.ds(0, count)]
    return pltpu.make_async_copy(part, part, sem)


def kernel(
    owners_hbm, x_hbm, out, owners, inverse, found, x_in, sums, means, rows, energy, plane,
    plane_sum, line, scales, ahead, early, split_a, split_b, mixed_a, mixed_b, sorted_a, sorted_b, got_a, got_b,
    in_sem, own_sem, y_sem, plane_send, plane_recv, line_send, line_recv,
    scale_send, scale_recv, early_send, early_recv,
    one_send, one_recv, two_send, two_recv,
):
    layers, tokens, features = x_in.shape
    octets, slices = tokens // 8, features // LANES
    section, column = lax.axis_index("section"), lax.axis_index("dp")
    y, zh = lax.div(section, 2), lax.rem(section, 2)
    zl, slot = lax.div(column, 8), lax.rem(column, 8)
    z = zh * 4 + zl
    x, c = lax.div(slot, 2), lax.rem(slot, 2)
    me = section * 32 + column
    split, mixed = (split_a, split_b), (mixed_a, mixed_b)
    ordered, got = (sorted_a, sorted_b), (got_a, got_b)

    loads = [
        pltpu.make_async_copy(x_hbm.at[i], x_in.at[i], in_sem.at[i]) for i in range(layers)
    ]
    for load in loads:
        load.start()
    fetch = pltpu.make_async_copy(owners_hbm, owners, own_sem.at[0])
    fetch.start()

    def signal(sem, target):
        pl.semaphore_signal(sem, inc=1, device_id=device(target), device_id_type=MESH)

    barrier = pltpu.get_barrier_semaphore()
    for step in (3, 5, 2, 6, 1, 7):
        signal(barrier, y * 64 + lax.rem(z + step, 8) * 8 + slot)
    for step in (2, 1, 3):
        signal(barrier, lax.rem(y + step, 4) * 64 + z * 8 + slot)
    for step in (1, 7):
        signal(barrier, y * 64 + lax.rem(z + step, 8) * 8 + x * 2 + 1 - c)
    for step in range(1, 8):
        signal(barrier, y * 64 + z * 8 + lax.rem(slot + step, 8))

    for layer in range(layers):
        loads[layer].wait()

        def add_up(q, _, layer=layer):
            at = pl.ds(pl.multiple_of(q * 8, 8), 8)
            parts = [x_in[layer, at, j * LANES : (j + 1) * LANES] for j in range(slices)]
            while len(parts) > 1:
                parts = [a + b for a, b in zip(parts[::2], parts[1::2])]
            sums[layer * octets + q] = parts[0]
            return 0

        lax.fori_loop(0, octets, add_up, 0)
    mean = jnp.sum(sums[...], axis=2, keepdims=True) / features
    means[...] = jnp.broadcast_to(mean, means.shape)

    for layer in range(layers):

        def squares(q, totals, layer=layer):
            at = pl.ds(pl.multiple_of(q * 8, 8), 8)
            mean = means[layer * octets + q]
            totals = list(totals)
            for j in range(slices):
                piece = x_in[layer, at, j * LANES : (j + 1) * LANES] - mean
                totals[j % 4] = totals[j % 4] + piece * piece
            return tuple(totals)

        zero = jnp.zeros((8, LANES), F32)
        totals = lax.fori_loop(0, octets, squares, (zero,) * 4)
        total = (totals[0] + totals[1]) + (totals[2] + totals[3])
        summed = jnp.sum(total, axis=0, keepdims=True)
        energy[layer : layer + 1, :] = summed
        energy[layer + 4 : layer + 5, :] = summed

    plane[slot] = energy[...]
    pl.semaphore_wait(barrier, 18)
    for step in range(1, 8):
        pltpu.make_async_remote_copy(
            energy, plane.at[slot], plane_send, plane_recv,
            device_id=device(y * 64 + z * 8 + lax.rem(slot + step, 8)), device_id_type=MESH,
        ).start()

    def arrange(j, into):
        lanes = pl.ds(pl.multiple_of(j * LANES, LANES), LANES)
        for layer in range(layers):
            for q in range(octets):
                piece = x_in[layer, q * 8 : q * 8 + 8, lanes] - means[layer * octets + q]
                into[q, pl.ds(layer, 8, stride=4), :] = piece

    def slot_at(dx, dc):
        return lax.rem(x + dx, 4) * 2 + lax.rem(c + dc, 2)

    def send_early(steps):
        for k in steps:
            there = slot_at(*EARLY[k])
            for i, (away, move) in enumerate(((1, 1), (3, 7))):
                source = rows.at[lax.rem(zl + away, 4) * 8 + there]
                pltpu.make_async_remote_copy(
                    ahead.at[2 * k + i] if k < FIRST else source, early.at[2 * k + i],
                    early_send, early_recv,
                    device_id=device(y * 64 + lax.rem(z + move, 8) * 8 + there),
                    device_id_type=MESH,
                ).start()

    for k in range(FIRST):
        for i, away in enumerate((1, 3)):
            arrange(lax.rem(zl + away, 4) * 8 + slot_at(*EARLY[k]), ahead.at[2 * k + i])
    send_early(range(FIRST))

    def arrange_all(j, _):
        arrange(j, rows.at[j])
        return 0

    lax.fori_loop(0, slices, arrange_all, 0)

    whole(plane, 7, plane_recv).wait()
    partial = plane[0]
    for i in range(1, 8):
        partial = partial + plane[i]
    plane_sum[...] = partial
    line[zl] = partial
    for step in (3, 2, 1):
        pltpu.make_async_remote_copy(
            plane_sum, line.at[zl], line_send, line_recv,
            device_id=device(y * 64 + zh * 32 + lax.rem(zl + step, 4) * 8 + slot), device_id_type=MESH,
        ).start()
    send_early(range(FIRST, len(EARLY)))
    for step in (2, 1, 3):
        signal(y_sem, lax.rem(y + step, 4) * 64 + z * 8 + slot)
    fetch.wait()
    numbers = (
        lax.broadcasted_iota(jnp.int32, (8, LANES), 0) * LANES
        + lax.broadcasted_iota(jnp.int32, (8, LANES), 1)
    )

    def invert(b, known):
        return jnp.where(numbers == owners[b], b, known)

    found[...] = lax.fori_loop(0, 256, invert, jnp.zeros((8, LANES), jnp.int32), unroll=8)
    table = pltpu.make_async_copy(found, inverse, own_sem.at[1])
    table.start()
    whole(line, 3, line_recv).wait()
    total = (line[0] + line[1]) + (line[2] + line[3])
    total = jnp.sum(total, axis=1, keepdims=True)
    scale = 1.0 / jnp.sqrt(total / (tokens * 32 * features) + 1.0)
    scale = jnp.broadcast_to(scale, (8, LANES))
    scales[2] = scale

    my_blocks = pl.ds(pl.multiple_of(column * 8, 8), 8)
    for h in range(2):
        if h == 1: whole(mixed[0], LATE, one_send.at[0]).wait()
        for away in (2, 1, 3, 0):
            first = lax.rem(zl + away, 4) * 8

            def pack(i, _, h=h, first=first):
                for q in range(octets):
                    for k in range(2):
                        piece = rows[first + i, q, pl.ds(16 * k + 8 * h, 8), :] * scale
                        split[h][first + i, 2 * q + k] = piece.astype(BF16)
                return 0

            lax.fori_loop(0, 8, pack, 0)
            if h == 0 and away == 2:
                for i, move in enumerate((1, 7)):
                    pltpu.make_async_remote_copy(
                        scales.at[2], scales.at[i], scale_send, scale_recv,
                        device_id=device(y * 64 + lax.rem(z + move, 8) * 8 + slot),
                        device_id_type=MESH,
                    ).start()
            for dx, dc in ((2, 0), (2, 1), (1, 0), (3, 0), (1, 1), (3, 1), (0, 1), (0, 0)):
                if (away == 0 and dx + dc == 0) or (away in (1, 3) and (dx, dc) in EARLY):
                    continue
                there = slot_at(dx, dc)
                if away == 2:
                    tz = lax.rem(z + 2 + 4 * ((dx + h) % 2), 8)
                else:
                    tz = lax.rem(z + (0, 1, 2, 7)[away], 8)
                pltpu.make_async_remote_copy(
                    split[h].at[first + there], mixed[h].at[my_blocks],
                    one_send.at[h], one_recv.at[h],
                    device_id=device(y * 64 + tz * 8 + there), device_id_type=MESH,
                ).start()
        mixed[h][my_blocks] = split[h][column]

    table.wait()
    pl.semaphore_wait(y_sem, 3)
    whole(scales, 2, scale_recv).wait()
    whole(early, 2 * len(EARLY), early_recv).wait()
    for h in range(2):
        for k, (dx, dc) in enumerate(EARLY):
            for i, away in enumerate((3, 1)):
                source = lax.rem(zl + away, 4) * 8 + slot_at((4 - dx) % 4, dc)
                for q in range(octets):
                    for part in range(2):
                        low = 16 * part + 8 * h
                        piece = early[2 * k + i, q, low : low + 8, :] * scales[i]
                        mixed[h][source * 8 + 2 * q + part] = piece.astype(BF16)
        whole(mixed[h], LATE, one_recv.at[h]).wait()
        for top in range(2):

            def order(o, _, h=h, top=top):
                ordered[h][top * LANES + o] = mixed[h][inverse[top, o]]
                return 0

            lax.fori_loop(0, LANES, order, 0, unroll=8)

        def send_two(tz, offset, h=h):
            across = lax.rem(y * 8 + slot + offset, 32)
            ty, there = lax.div(across, 8), lax.rem(across, 8)
            target = ty * 64 + tz * 8 + there

            @pl.when(target != me)
            def _():
                to = {"section": ty * 2 + lax.div(tz, 4), "dp": lax.rem(tz, 4) * 8 + there}
                pltpu.make_async_remote_copy(
                    ordered[h].at[target], got[h].at[me], two_send.at[h], two_recv.at[h],
                    device_id=to, device_id_type=MESH,
                ).start()

        def send_mixed(i, _):
            for k in range(RATE):
                n = i * RATE + k
                send_two(lax.rem(n, FRONT), lax.div(n, FRONT))
            for tz in range(FRONT, 8):
                send_two(tz, i)
            return 0

        def send_rest(i, _):
            for tz in range(FRONT, 8):
                send_two(tz, i)
            return 0

        steps = FRONT * 32 // RATE
        lax.fori_loop(0, steps, send_mixed, 0)
        lax.fori_loop(steps, 32, send_rest, 0)
        got[h][me] = ordered[h][me]

    block = inverse[lax.div(me, LANES), lax.rem(me, LANES)]
    from_z, from_x = lax.div(block, 64), lax.rem(lax.div(block, 2 * 8), 4)
    low = lax.broadcasted_iota(jnp.int32, (8, LANES), 0) < 4
    for h in range(2):
        whole(got[h], 255, two_recv.at[h]).wait()

        def place(there, _, h=h):
            away = lax.rem(there - from_z + 4, 4)
            for odd in range(2):
                far = lax.rem(odd + from_x + h, 2)
                move = jnp.where(away == 3, 7, jnp.where(away == 2, 2 + 4 * far, away))
                half = lax.div(lax.rem(from_z + move, 8), 4)
                for k in range(4):
                    near_at = k * 64 + half * 32 + there * 8
                    far_at = k * 64 + (1 - half) * 32 + there * 8
                    for i in (2 * odd, 2 * odd + 1, 2 * odd + 4, 2 * odd + 5):
                        at = pl.ds(pl.multiple_of((there * 8 + i) * LANES, LANES), LANES)
                        first = got[h][near_at + i].astype(F32)
                        second = got[h][far_at + i].astype(F32)
                        upper = jnp.where(low, first, pltpu.roll(second, 4, 0))
                        lower = jnp.where(low, pltpu.roll(first, 4, 0), second)
                        out[2 * h, pl.ds(8 * k, 8), at] = upper.astype(BF16)
                        out[2 * h + 1, pl.ds(8 * k, 8), at] = lower.astype(BF16)
            return 0

        lax.fori_loop(0, 4, place, 0)

    whole(plane, 7, plane_send).wait()
    whole(line, 3, line_send).wait()
    whole(scales, 2, scale_send).wait()
    whole(early, 2 * len(EARLY), early_send).wait()
    for h in range(2):
        if h == 1: whole(mixed[h], LATE, one_send.at[h]).wait()
        whole(got[h], 255, two_send.at[h]).wait()


def on_device(residuals, owners):
    layers, tokens, features = residuals.shape
    blocks = owners.shape[0]
    dma, vmem = pltpu.SemaphoreType.DMA, pltpu.VMEM
    tile = vmem((8, LANES), F32)
    pieces = vmem((blocks, 8, LANES), BF16)
    octets = layers * tokens // 8
    return pl.pallas_call(
        kernel,
        out_shape=jax.ShapeDtypeStruct((4, 8 * layers, features), BF16),
        in_specs=[pl.BlockSpec(memory_space=pltpu.HBM)] * 2,
        out_specs=pl.BlockSpec(memory_space=pltpu.VMEM),
        scratch_shapes=[
            pltpu.SMEM((blocks,), jnp.int32),
            pltpu.SMEM((8, LANES), jnp.int32),
            vmem((8, LANES), jnp.int32),
            vmem((layers, tokens, features), F32),
            vmem((octets, 8, LANES), F32),
            vmem((octets, 8, LANES), F32),
            vmem((features // LANES, tokens // 8, 32, LANES), F32),
            tile,
            vmem((8, 8, LANES), F32),
            tile,
            vmem((4, 8, LANES), F32),
            vmem((3, 8, LANES), F32),
            vmem((2 * FIRST, tokens // 8, 32, LANES), F32),
            vmem((2 * len(EARLY), tokens // 8, 32, LANES), F32),
            vmem((32, 8, 8, LANES), BF16),
            vmem((32, 8, 8, LANES), BF16),
            pieces, pieces, pieces, pieces, pieces, pieces,
            dma((layers,)),
            dma((2,)),
            pltpu.SemaphoreType.REGULAR,
            dma, dma, dma, dma, dma, dma, dma, dma,
            dma((2,)), dma((2,)), dma((2,)), dma((2,)),
        ],
        compiler_params=pltpu.CompilerParams(
            collective_id=0, has_side_effects=True, vmem_limit_bytes=16 * 2**20
        ),
    )(*(pltpu.with_memory_space_constraint(a, pltpu.HBM) for a in (owners, residuals)))


def solution(mesh):
    return jax.shard_map(
        on_device,
        mesh=mesh,
        in_specs=(P("section", "dp", None), P()),
        out_specs=P(("section", "dp"), None, None),
        check_vma=False,
    )
```

```python
import jax
import jax.numpy as jnp
from jax import lax
from jax.experimental import pallas as pl
from jax.experimental.pallas import tpu as pltpu
from jax.sharding import PartitionSpec as P

MESH = pl.DeviceIdType.MESH
F32 = jnp.float32
BF16 = jnp.bfloat16
LANES = 128
EARLY = ((0, 0), (0, 1), (1, 0), (3, 1))
FIRST = 2
FRONT = 1
RATE = 2
LATE = 248 - 16 * len(EARLY)


def device(number):
    return {"section": lax.div(number, 32), "dp": lax.rem(number, 32)}


def whole(ref, count, sem):
    part = ref.at[pl.ds(0, count)]
    return pltpu.make_async_copy(part, part, sem)


def kernel(
    owners_hbm, x_hbm, out, owners, inverse, found, x_in, sums, means, rows, energy, plane,
    plane_sum, line, scales, ahead, early, split_a, split_b, mixed_a, mixed_b, sorted_a, sorted_b, got_a, got_b,
    in_sem, own_sem, y_sem, plane_send, plane_recv, line_send, line_recv,
    scale_send, scale_recv, early_send, early_recv,
    one_send, one_recv, two_send, two_recv,
):
    layers, tokens, features = x_in.shape
    octets, slices = tokens // 8, features // LANES
    section, column = lax.axis_index("section"), lax.axis_index("dp")
    y, zh = lax.div(section, 2), lax.rem(section, 2)
    zl, slot = lax.div(column, 8), lax.rem(column, 8)
    z = zh * 4 + zl
    x, c = lax.div(slot, 2), lax.rem(slot, 2)
    me = section * 32 + column
    split, mixed = (split_a, split_b), (mixed_a, mixed_b)
    ordered, got = (sorted_a, sorted_b), (got_a, got_b)

    loads = [
        pltpu.make_async_copy(x_hbm.at[i], x_in.at[i], in_sem.at[i]) for i in range(layers)
    ]
    for load in loads:
        load.start()
    fetch = pltpu.make_async_copy(owners_hbm, owners, own_sem.at[0])
    fetch.start()

    def signal(sem, target):
        pl.semaphore_signal(sem, inc=1, device_id=device(target), device_id_type=MESH)

    barrier = pltpu.get_barrier_semaphore()
    for step in (4, 5, 3, 2, 6, 7, 1):
        signal(barrier, y * 64 + z * 8 + lax.rem(slot + step, 8))
    for step in (3, 5, 2, 6, 1, 7):
        signal(barrier, y * 64 + lax.rem(z + step, 8) * 8 + slot)
    for step in (2, 1, 3):
        signal(barrier, lax.rem(y + step, 4) * 64 + z * 8 + slot)
    for step in (1, 7):
        signal(barrier, y * 64 + lax.rem(z + step, 8) * 8 + x * 2 + 1 - c)

    for layer in range(layers):
        loads[layer].wait()

        def add_up(q, _, layer=layer):
            at = pl.ds(pl.multiple_of(q * 8, 8), 8)
            parts = [x_in[layer, at, j * LANES : (j + 1) * LANES] for j in range(slices)]
            while len(parts) > 1:
                parts = [a + b for a, b in zip(parts[::2], parts[1::2])]
            sums[layer * octets + q] = parts[0]
            return 0

        lax.fori_loop(0, octets, add_up, 0)
    mean = jnp.sum(sums[...], axis=2, keepdims=True) / features
    means[...] = jnp.broadcast_to(mean, means.shape)

    for layer in range(layers):

        def squares(q, totals, layer=layer):
            at = pl.ds(pl.multiple_of(q * 8, 8), 8)
            mean = means[layer * octets + q]
            totals = list(totals)
            for j in range(slices):
                piece = x_in[layer, at, j * LANES : (j + 1) * LANES] - mean
                totals[j % 4] = totals[j % 4] + piece * piece
            return tuple(totals)

        zero = jnp.zeros((8, LANES), F32)
        totals = lax.fori_loop(0, octets, squares, (zero,) * 4)
        total = (totals[0] + totals[1]) + (totals[2] + totals[3])
        summed = jnp.sum(total, axis=0, keepdims=True)
        energy[layer : layer + 1, :] = summed

    plane[slot] = energy[...]
    pl.semaphore_wait(barrier, 18)
    for step in (4, 5, 3, 2, 6, 7, 1):
        pltpu.make_async_remote_copy(
            energy, plane.at[slot], plane_send, plane_recv,
            device_id=device(y * 64 + z * 8 + lax.rem(slot + step, 8)), device_id_type=MESH,
        ).start()

    def arrange(j, into):
        lanes = pl.ds(pl.multiple_of(j * LANES, LANES), LANES)
        for layer in range(layers):
            for q in range(octets):
                piece = x_in[layer, q * 8 : q * 8 + 8, lanes] - means[layer * octets + q]
                into[q, pl.ds(layer, 8, stride=4), :] = piece

    def slot_at(dx, dc):
        return lax.rem(x + dx, 4) * 2 + lax.rem(c + dc, 2)

    def send_early(steps):
        for k in steps:
            there = slot_at(*EARLY[k])
            for i, (away, move) in enumerate(((1, 1), (3, 7))):
                source = rows.at[lax.rem(zl + away, 4) * 8 + there]
                pltpu.make_async_remote_copy(
                    ahead.at[2 * k + i] if k < FIRST else source, early.at[2 * k + i],
                    early_send, early_recv,
                    device_id=device(y * 64 + lax.rem(z + move, 8) * 8 + there),
                    device_id_type=MESH,
                ).start()

    for k in range(FIRST):
        for i, away in enumerate((1, 3)):
            arrange(lax.rem(zl + away, 4) * 8 + slot_at(*EARLY[k]), ahead.at[2 * k + i])
    send_early(range(FIRST))

    def arrange_all(j, _):
        arrange(j, rows.at[j])
        return 0

    lax.fori_loop(0, slices, arrange_all, 0)

    whole(plane, 7, plane_recv).wait()
    partial = plane[0]
    for i in range(1, 8):
        partial = partial + plane[i]
    plane_sum[...] = partial
    line[zl] = partial
    for step in (3, 2, 1):
        pltpu.make_async_remote_copy(
            plane_sum, line.at[zl], line_send, line_recv,
            device_id=device(y * 64 + zh * 32 + lax.rem(zl + step, 4) * 8 + slot), device_id_type=MESH,
        ).start()
    send_early(range(FIRST, len(EARLY)))
    for step in (2, 1, 3):
        signal(y_sem, lax.rem(y + step, 4) * 64 + z * 8 + slot)
    fetch.wait()
    numbers = (
        lax.broadcasted_iota(jnp.int32, (8, LANES), 0) * LANES
        + lax.broadcasted_iota(jnp.int32, (8, LANES), 1)
    )

    def invert(b, known):
        return jnp.where(numbers == owners[b], b, known)

    found[...] = lax.fori_loop(0, 256, invert, jnp.zeros((8, LANES), jnp.int32), unroll=8)
    table = pltpu.make_async_copy(found, inverse, own_sem.at[1])
    table.start()
    whole(line, 3, line_recv).wait()
    total = (line[0] + line[1]) + (line[2] + line[3])
    total = jnp.sum(jnp.concatenate([total, total], axis=0), axis=1, keepdims=True)
    scale = 1.0 / jnp.sqrt(total / (tokens * 32 * features) + 1.0)
    scale = jnp.broadcast_to(scale, (8, LANES))
    scales[2] = scale

    my_blocks = pl.ds(pl.multiple_of(column * 8, 8), 8)
    for h in range(2):
        if h == 1: whole(mixed[0], LATE, one_send.at[0]).wait()
        for away in (2, 1, 3, 0):
            first = lax.rem(zl + away, 4) * 8

            def pack(i, _, h=h, first=first):
                for q in range(octets):
                    for k in range(2):
                        piece = rows[first + i, q, pl.ds(16 * k + 8 * h, 8), :] * scale
                        split[h][first + i, 2 * q + k] = piece.astype(BF16)
                return 0

            lax.fori_loop(0, 8, pack, 0)
            if h == 0 and away == 2:
                for i, move in enumerate((1, 7)):
                    pltpu.make_async_remote_copy(
                        scales.at[2], scales.at[i], scale_send, scale_recv,
                        device_id=device(y * 64 + lax.rem(z + move, 8) * 8 + slot),
                        device_id_type=MESH,
                    ).start()
            for dx, dc in ((2, 0), (2, 1), (1, 0), (3, 0), (1, 1), (3, 1), (0, 1), (0, 0)):
                if (away == 0 and dx + dc == 0) or (away in (1, 3) and (dx, dc) in EARLY):
                    continue
                there = slot_at(dx, dc)
                if away == 2:
                    tz = lax.rem(z + 2 + 4 * ((dx + h) % 2), 8)
                else:
                    tz = lax.rem(z + (0, 1, 2, 7)[away], 8)
                pltpu.make_async_remote_copy(
                    split[h].at[first + there], mixed[h].at[my_blocks],
                    one_send.at[h], one_recv.at[h],
                    device_id=device(y * 64 + tz * 8 + there), device_id_type=MESH,
                ).start()
        mixed[h][my_blocks] = split[h][column]

    table.wait()
    pl.semaphore_wait(y_sem, 3)
    whole(scales, 2, scale_recv).wait()
    whole(early, 2 * len(EARLY), early_recv).wait()
    for h in range(2):
        for k, (dx, dc) in enumerate(EARLY):
            for i, away in enumerate((3, 1)):
                source = lax.rem(zl + away, 4) * 8 + slot_at((4 - dx) % 4, dc)
                for q in range(octets):
                    for part in range(2):
                        low = 16 * part + 8 * h
                        piece = early[2 * k + i, q, low : low + 8, :] * scales[i]
                        mixed[h][source * 8 + 2 * q + part] = piece.astype(BF16)
        whole(mixed[h], LATE, one_recv.at[h]).wait()
        for top in range(2):

            def order(o, _, h=h, top=top):
                ordered[h][top * LANES + o] = mixed[h][inverse[top, o]]
                return 0

            lax.fori_loop(0, LANES, order, 0, unroll=8)

        def send_two(tz, offset, h=h):
            across = lax.rem(y * 8 + slot + offset, 32)
            ty, there = lax.div(across, 8), lax.rem(across, 8)
            target = ty * 64 + tz * 8 + there

            @pl.when(target != me)
            def _():
                to = {"section": ty * 2 + lax.div(tz, 4), "dp": lax.rem(tz, 4) * 8 + there}
                pltpu.make_async_remote_copy(
                    ordered[h].at[target], got[h].at[me], two_send.at[h], two_recv.at[h],
                    device_id=to, device_id_type=MESH,
                ).start()

        def send_mixed(i, _):
            for k in range(RATE):
                n = i * RATE + k
                send_two(lax.rem(n, FRONT), lax.div(n, FRONT))
            for tz in range(FRONT, 8):
                send_two(tz, i)
            return 0

        def send_rest(i, _):
            for tz in range(FRONT, 8):
                send_two(tz, i)
            return 0

        steps = FRONT * 32 // RATE
        lax.fori_loop(0, steps, send_mixed, 0)
        lax.fori_loop(steps, 32, send_rest, 0)
        got[h][me] = ordered[h][me]

    block = inverse[lax.div(me, LANES), lax.rem(me, LANES)]
    from_z, from_x = lax.div(block, 64), lax.rem(lax.div(block, 2 * 8), 4)
    low = lax.broadcasted_iota(jnp.int32, (8, LANES), 0) < 4
    for h in range(2):
        whole(got[h], 255, two_recv.at[h]).wait()

        def place(there, _, h=h):
            away = lax.rem(there - from_z + 4, 4)
            for odd in range(2):
                far = lax.rem(odd + from_x + h, 2)
                move = jnp.where(away == 3, 7, jnp.where(away == 2, 2 + 4 * far, away))
                half = lax.div(lax.rem(from_z + move, 8), 4)
                for k in range(4):
                    near_at = k * 64 + half * 32 + there * 8
                    far_at = k * 64 + (1 - half) * 32 + there * 8
                    for i in (2 * odd, 2 * odd + 1, 2 * odd + 4, 2 * odd + 5):
                        at = pl.ds(pl.multiple_of((there * 8 + i) * LANES, LANES), LANES)
                        first = got[h][near_at + i].astype(F32)
                        second = got[h][far_at + i].astype(F32)
                        upper = jnp.where(low, first, pltpu.roll(second, 4, 0))
                        lower = jnp.where(low, pltpu.roll(first, 4, 0), second)
                        out[2 * h, pl.ds(8 * k, 8), at] = upper.astype(BF16)
                        out[2 * h + 1, pl.ds(8 * k, 8), at] = lower.astype(BF16)
            return 0

        lax.fori_loop(0, 4, place, 0)

    whole(plane, 7, plane_send).wait()
    whole(line, 3, line_send).wait()
    whole(scales, 2, scale_send).wait()
    whole(early, 2 * len(EARLY), early_send).wait()
    for h in range(2):
        if h == 1: whole(mixed[h], LATE, one_send.at[h]).wait()
        whole(got[h], 255, two_send.at[h]).wait()


def on_device(residuals, owners):
    layers, tokens, features = residuals.shape
    blocks = owners.shape[0]
    dma, vmem = pltpu.SemaphoreType.DMA, pltpu.VMEM
    tile = vmem((8, LANES), F32)
    pieces = vmem((blocks, 8, LANES), BF16)
    octets = layers * tokens // 8
    return pl.pallas_call(
        kernel,
        out_shape=jax.ShapeDtypeStruct((4, 8 * layers, features), BF16),
        in_specs=[pl.BlockSpec(memory_space=pltpu.HBM)] * 2,
        out_specs=pl.BlockSpec(memory_space=pltpu.VMEM),
        scratch_shapes=[
            pltpu.SMEM((blocks,), jnp.int32),
            pltpu.SMEM((8, LANES), jnp.int32),
            vmem((8, LANES), jnp.int32),
            vmem((layers, tokens, features), F32),
            vmem((octets, 8, LANES), F32),
            vmem((octets, 8, LANES), F32),
            vmem((features // LANES, tokens // 8, 32, LANES), F32),
            vmem((layers, LANES), F32),
            vmem((8, layers, LANES), F32),
            vmem((layers, LANES), F32),
            vmem((4, layers, LANES), F32),
            vmem((3, 8, LANES), F32),
            vmem((2 * FIRST, tokens // 8, 32, LANES), F32),
            vmem((2 * len(EARLY), tokens // 8, 32, LANES), F32),
            vmem((32, 8, 8, LANES), BF16),
            vmem((32, 8, 8, LANES), BF16),
            pieces, pieces, pieces, pieces, pieces, pieces,
            dma((layers,)),
            dma((2,)),
            pltpu.SemaphoreType.REGULAR,
            dma, dma, dma, dma, dma, dma, dma, dma,
            dma((2,)), dma((2,)), dma((2,)), dma((2,)),
        ],
        compiler_params=pltpu.CompilerParams(
            collective_id=0, has_side_effects=True, vmem_limit_bytes=16 * 2**20
        ),
    )(*(pltpu.with_memory_space_constraint(a, pltpu.HBM) for a in (owners, residuals)))


def solution(mesh):
    return jax.shard_map(
        on_device,
        mesh=mesh,
        in_specs=(P("section", "dp", None), P()),
        out_specs=P(("section", "dp"), None, None),
        check_vma=False,
    )
```

```python
import jax
import jax.numpy as jnp
from jax import lax
from jax.experimental import pallas as pl
from jax.experimental.pallas import tpu as pltpu
from jax.sharding import PartitionSpec as P

MESH = pl.DeviceIdType.MESH
F32 = jnp.float32
BF16 = jnp.bfloat16
LANES = 128
EARLY = ((0, 0), (0, 1), (1, 0), (3, 1))
FIRST = 2
FRONT = 1
RATE = 2
LATE = 248 - 16 * len(EARLY)


def device(number):
    return {"section": lax.div(number, 32), "dp": lax.rem(number, 32)}


def whole(ref, count, sem):
    part = ref.at[pl.ds(0, count)]
    return pltpu.make_async_copy(part, part, sem)


def kernel(
    owners_hbm, x_hbm, out, owners, inverse, found, x_in, sums, means, rows, energy, plane,
    plane_sum, line, scales, ahead, early, split_a, split_b, mixed_a, mixed_b, sorted_a, sorted_b, got_a, got_b,
    in_sem, own_sem, y_sem, plane_send, plane_recv, line_send, line_recv,
    scale_send, scale_recv, early_send, early_recv,
    one_send, one_recv, two_send, two_recv,
):
    layers, tokens, features = x_in.shape
    octets, slices = tokens // 8, features // LANES
    section, column = lax.axis_index("section"), lax.axis_index("dp")
    y, zh = lax.div(section, 2), lax.rem(section, 2)
    zl, slot = lax.div(column, 8), lax.rem(column, 8)
    z = zh * 4 + zl
    x, c = lax.div(slot, 2), lax.rem(slot, 2)
    me = section * 32 + column
    split, mixed = (split_a, split_b), (mixed_a, mixed_b)
    ordered, got = (sorted_a, sorted_b), (got_a, got_b)

    loads = [
        pltpu.make_async_copy(x_hbm.at[i], x_in.at[i], in_sem.at[i]) for i in range(layers)
    ]
    for load in loads:
        load.start()
    fetch = pltpu.make_async_copy(owners_hbm, owners, own_sem.at[0])
    fetch.start()

    def signal(sem, target):
        pl.semaphore_signal(sem, inc=1, device_id=device(target), device_id_type=MESH)

    barrier = pltpu.get_barrier_semaphore()
    for step in (4, 5, 3, 2, 6, 7, 1):
        signal(barrier, y * 64 + z * 8 + lax.rem(slot + step, 8))
    for step in (3, 5, 2, 6, 1, 7):
        signal(barrier, y * 64 + lax.rem(z + step, 8) * 8 + slot)
    for step in (2, 1, 3):
        signal(barrier, lax.rem(y + step, 4) * 64 + z * 8 + slot)
    for step in (1, 7):
        signal(barrier, y * 64 + lax.rem(z + step, 8) * 8 + x * 2 + 1 - c)

    for layer in range(layers):
        loads[layer].wait()

        def add_up(q, _, layer=layer):
            at = pl.ds(pl.multiple_of(q * 8, 8), 8)
            parts = [x_in[layer, at, j * LANES : (j + 1) * LANES] for j in range(slices)]
            while len(parts) > 1:
                parts = [a + b for a, b in zip(parts[::2], parts[1::2])]
            sums[layer * octets + q] = parts[0]
            return 0

        lax.fori_loop(0, octets, add_up, 0)
    mean = jnp.sum(sums[...], axis=2, keepdims=True) / features
    means[...] = jnp.broadcast_to(mean, means.shape)

    for layer in range(layers):

        def squares(q, totals, layer=layer):
            at = pl.ds(pl.multiple_of(q * 8, 8), 8)
            mean = means[layer * octets + q]
            totals = list(totals)
            for j in range(slices):
                piece = x_in[layer, at, j * LANES : (j + 1) * LANES] - mean
                totals[j % 4] = totals[j % 4] + piece * piece
            return tuple(totals)

        zero = jnp.zeros((8, LANES), F32)
        totals = lax.fori_loop(0, octets, squares, (zero,) * 4)
        total = (totals[0] + totals[1]) + (totals[2] + totals[3])
        summed = jnp.sum(total, axis=0, keepdims=True)
        energy[layer : layer + 1, :] = summed

    plane[slot] = energy[...]
    pl.semaphore_wait(barrier, 18)
    for step in (4, 5, 3, 2, 6, 7, 1):
        pltpu.make_async_remote_copy(
            energy, plane.at[slot], plane_send, plane_recv,
            device_id=device(y * 64 + z * 8 + lax.rem(slot + step, 8)), device_id_type=MESH,
        ).start()

    def arrange(j, into):
        lanes = pl.ds(pl.multiple_of(j * LANES, LANES), LANES)
        for layer in range(layers):
            for q in range(octets):
                piece = x_in[layer, q * 8 : q * 8 + 8, lanes] - means[layer * octets + q]
                into[q, pl.ds(layer, 8, stride=4), :] = piece

    def slot_at(dx, dc):
        return lax.rem(x + dx, 4) * 2 + lax.rem(c + dc, 2)

    def send_early(steps):
        for k in steps:
            there = slot_at(*EARLY[k])
            for i, (away, move) in enumerate(((1, 1), (3, 7))):
                source = rows.at[lax.rem(zl + away, 4) * 8 + there]
                pltpu.make_async_remote_copy(
                    ahead.at[2 * k + i] if k < FIRST else source, early.at[2 * k + i],
                    early_send, early_recv,
                    device_id=device(y * 64 + lax.rem(z + move, 8) * 8 + there),
                    device_id_type=MESH,
                ).start()

    for k in range(FIRST):
        for i, away in enumerate((1, 3)):
            arrange(lax.rem(zl + away, 4) * 8 + slot_at(*EARLY[k]), ahead.at[2 * k + i])
    send_early(range(FIRST))

    def arrange_all(j, _):
        arrange(j, rows.at[j])
        return 0

    lax.fori_loop(0, slices, arrange_all, 0)

    whole(plane, 7, plane_recv).wait()
    partial = plane[0]
    for i in range(1, 8):
        partial = partial + plane[i]
    plane_sum[...] = partial
    line[zl] = partial
    for step in (3, 2, 1):
        pltpu.make_async_remote_copy(
            plane_sum, line.at[zl], line_send, line_recv,
            device_id=device(y * 64 + zh * 32 + lax.rem(zl + step, 4) * 8 + slot), device_id_type=MESH,
        ).start()
    send_early(range(FIRST, len(EARLY)))
    for step in (2, 1, 3):
        signal(y_sem, lax.rem(y + step, 4) * 64 + z * 8 + slot)
    fetch.wait()
    numbers = (
        lax.broadcasted_iota(jnp.int32, (8, LANES), 0) * LANES
        + lax.broadcasted_iota(jnp.int32, (8, LANES), 1)
    )

    def invert(b, known):
        return jnp.where(numbers == owners[b], b, known)

    found[...] = lax.fori_loop(0, 256, invert, jnp.zeros((8, LANES), jnp.int32), unroll=8)
    table = pltpu.make_async_copy(found, inverse, own_sem.at[1])
    table.start()
    whole(line, 3, line_recv).wait()
    total = (line[0] + line[1]) + (line[2] + line[3])
    total = jnp.sum(jnp.concatenate([total, total], axis=0), axis=1, keepdims=True)
    scale = 1.0 / jnp.sqrt(total / (tokens * 32 * features) + 1.0)
    scale = jnp.broadcast_to(scale, (8, LANES))
    scales[2] = scale

    my_blocks = pl.ds(pl.multiple_of(column * 8, 8), 8)
    for h in range(2):
        if h == 1: whole(mixed[0], LATE, one_send.at[0]).wait()
        for away in (2, 1, 3, 0):
            first = lax.rem(zl + away, 4) * 8

            def pack(i, _, h=h, first=first):
                for q in range(octets):
                    for k in range(2):
                        piece = rows[first + i, q, pl.ds(16 * k + 8 * h, 8), :] * scale
                        split[h][first + i, 2 * q + k] = piece.astype(BF16)
                return 0

            lax.fori_loop(0, 8, pack, 0)
            if h == 0 and away == 2:
                for i, move in enumerate((1, 7)):
                    pltpu.make_async_remote_copy(
                        scales.at[2], scales.at[i], scale_send, scale_recv,
                        device_id=device(y * 64 + lax.rem(z + move, 8) * 8 + slot),
                        device_id_type=MESH,
                    ).start()
            for dx, dc in ((2, 0), (2, 1), (1, 0), (3, 0), (1, 1), (3, 1), (0, 1), (0, 0)):
                if (away == 0 and dx + dc == 0) or (away in (1, 3) and (dx, dc) in EARLY):
                    continue
                there = slot_at(dx, dc)
                if away == 2:
                    tz = lax.rem(z + 2 + 4 * ((dx + h) % 2), 8)
                else:
                    tz = lax.rem(z + (0, 1, 2, 7)[away], 8)
                pltpu.make_async_remote_copy(
                    split[h].at[first + there], mixed[h].at[my_blocks],
                    one_send.at[h], one_recv.at[h],
                    device_id=device(y * 64 + tz * 8 + there), device_id_type=MESH,
                ).start()
        mixed[h][my_blocks] = split[h][column]

    table.wait()
    pl.semaphore_wait(y_sem, 3)
    whole(scales, 2, scale_recv).wait()
    whole(early, 2 * len(EARLY), early_recv).wait()
    for h in range(2):
        for k, (dx, dc) in enumerate(EARLY):
            for i, away in enumerate((3, 1)):
                source = lax.rem(zl + away, 4) * 8 + slot_at((4 - dx) % 4, dc)
                for q in range(octets):
                    for part in range(2):
                        low = 16 * part + 8 * h
                        piece = early[2 * k + i, q, low : low + 8, :] * scales[i]
                        mixed[h][source * 8 + 2 * q + part] = piece.astype(BF16)
        whole(mixed[h], LATE, one_recv.at[h]).wait()
        for top in range(2):

            def order(o, _, h=h, top=top):
                ordered[h][top * LANES + o] = mixed[h][inverse[top, o]]
                return 0

            lax.fori_loop(0, LANES, order, 0, unroll=8)

        def send_two(tz, offset, h=h):
            across = lax.rem(y * 8 + slot + offset, 32)
            ty, there = lax.div(across, 8), lax.rem(across, 8)
            target = ty * 64 + tz * 8 + there

            @pl.when(target != me)
            def _():
                to = {"section": ty * 2 + lax.div(tz, 4), "dp": lax.rem(tz, 4) * 8 + there}
                pltpu.make_async_remote_copy(
                    ordered[h].at[target], got[h].at[me], two_send.at[h], two_recv.at[h],
                    device_id=to, device_id_type=MESH,
                ).start()

        def send_mixed(i, _):
            for k in range(RATE):
                n = i * RATE + k
                send_two(lax.rem(n, FRONT), lax.div(n, FRONT))
            for tz in range(FRONT, 8):
                send_two(tz, i)
            return 0

        def send_rest(i, _):
            for tz in range(FRONT, 8):
                send_two(tz, i)
            return 0

        steps = FRONT * 32 // RATE
        lax.fori_loop(0, steps, send_mixed, 0)
        lax.fori_loop(steps, 32, send_rest, 0)
        got[h][me] = ordered[h][me]

    block = inverse[lax.div(me, LANES), lax.rem(me, LANES)]
    from_z, from_x = lax.div(block, 64), lax.rem(lax.div(block, 2 * 8), 4)
    low = lax.broadcasted_iota(jnp.int32, (8, LANES), 0) < 4
    for h in range(2):
        whole(got[h], 255, two_recv.at[h]).wait()

        def place(there, _, h=h):
            away = lax.rem(there - from_z + 4, 4)
            for odd in range(2):
                far = lax.rem(odd + from_x + h, 2)
                move = jnp.where(away == 3, 7, jnp.where(away == 2, 2 + 4 * far, away))
                half = lax.div(lax.rem(from_z + move, 8), 4)
                for k in range(4):
                    near_at = k * 64 + half * 32 + there * 8
                    far_at = k * 64 + (1 - half) * 32 + there * 8
                    for i in (2 * odd, 2 * odd + 1, 2 * odd + 4, 2 * odd + 5):
                        at = pl.ds(pl.multiple_of((there * 8 + i) * LANES, LANES), LANES)
                        first = got[h][near_at + i].astype(F32)
                        second = got[h][far_at + i].astype(F32)
                        upper = jnp.where(low, first, pltpu.roll(second, 4, 0))
                        lower = jnp.where(low, pltpu.roll(first, 4, 0), second)
                        out[2 * h, pl.ds(8 * k, 8), at] = upper.astype(BF16)
                        out[2 * h + 1, pl.ds(8 * k, 8), at] = lower.astype(BF16)
            return 0

        lax.fori_loop(0, 4, place, 0)

    whole(plane, 7, plane_send).wait()
    whole(line, 3, line_send).wait()
    whole(scales, 2, scale_send).wait()
    whole(early, 2 * len(EARLY), early_send).wait()
    for h in range(2):
        if h == 1: whole(mixed[h], LATE, one_send.at[h]).wait()
        whole(got[h], 255, two_send.at[h]).wait()


def write_out(placed, out, sem):
    copies = [
        pltpu.make_async_copy(placed.at[i // 2, pl.ds(16 * (i % 2), 16)], out.at[i // 2, pl.ds(16 * (i % 2), 16)], sem.at[i])
        for i in range(8)
    ]
    for copy in copies:
        copy.start()
    for copy in copies:
        copy.wait()


def on_device(residuals, owners):
    layers, tokens, features = residuals.shape
    blocks = owners.shape[0]
    dma, vmem = pltpu.SemaphoreType.DMA, pltpu.VMEM
    tile = vmem((8, LANES), F32)
    pieces = vmem((blocks, 8, LANES), BF16)
    octets = layers * tokens // 8
    placed = pl.pallas_call(
        kernel,
        out_shape=jax.ShapeDtypeStruct((4, 8 * layers, features), BF16),
        in_specs=[pl.BlockSpec(memory_space=pltpu.HBM)] * 2,
        out_specs=pl.BlockSpec(memory_space=pltpu.VMEM),
        scratch_shapes=[
            pltpu.SMEM((blocks,), jnp.int32),
            pltpu.SMEM((8, LANES), jnp.int32),
            vmem((8, LANES), jnp.int32),
            vmem((layers, tokens, features), F32),
            vmem((octets, 8, LANES), F32),
            vmem((octets, 8, LANES), F32),
            vmem((features // LANES, tokens // 8, 32, LANES), F32),
            vmem((layers, LANES), F32),
            vmem((8, layers, LANES), F32),
            vmem((layers, LANES), F32),
            vmem((4, layers, LANES), F32),
            vmem((3, 8, LANES), F32),
            vmem((2 * FIRST, tokens // 8, 32, LANES), F32),
            vmem((2 * len(EARLY), tokens // 8, 32, LANES), F32),
            vmem((32, 8, 8, LANES), BF16),
            vmem((32, 8, 8, LANES), BF16),
            pieces, pieces, pieces, pieces, pieces, pieces,
            dma((layers,)),
            dma((2,)),
            pltpu.SemaphoreType.REGULAR,
            dma, dma, dma, dma, dma, dma, dma, dma,
            dma((2,)), dma((2,)), dma((2,)), dma((2,)),
        ],
        compiler_params=pltpu.CompilerParams(
            collective_id=0, has_side_effects=True, vmem_limit_bytes=16 * 2**20
        ),
    )(*(pltpu.with_memory_space_constraint(a, pltpu.HBM) for a in (owners, residuals)))
    return pl.pallas_call(
        write_out,
        out_shape=jax.ShapeDtypeStruct(placed.shape, placed.dtype),
        in_specs=[pl.BlockSpec(memory_space=pltpu.VMEM)],
        out_specs=pl.BlockSpec(memory_space=pltpu.HBM),
        scratch_shapes=[dma((8,))],
        compiler_params=pltpu.CompilerParams(vmem_limit_bytes=16 * 2**20),
    )(placed)


def solution(mesh):
    return jax.shard_map(
        on_device,
        mesh=mesh,
        in_specs=(P("section", "dp", None), P()),
        out_specs=P(("section", "dp"), None, None),
        check_vma=False,
    )
```
